32 devices in a mesh: chan: 4 (over x, core), tok: 8 (over z, y).
Axes of the slice: x: 2, y: 2, z: 4, core: 2. Of those that a mesh axis runs over, the one named last changes fastest.
Arguments:
- codes: bfloat16 [9600, 16384], P('tok', 'chan'), may hold values from -6 to 6
- scale_exp: int32 [16384], P('chan'), may hold values from -2 to 2
- delta: bfloat16 [9600, 16384], P('tok', 'chan'), may hold values from -4 to 4
Outputs:
- gram: float32 [16384, 128], P(('chan', 'tok'))
- mismatch: float32 [16384, 128], P(('chan', 'tok'))
The draws below stay inside these ranges and needn't reach their ends.
All inputs are finite; a program needn't handle non-finite values.
Results may differ from the reference program's by a relative error of at most 0.0003.
Values may be sent and summed in bfloat16 or wider, within the bound.
No kernel may reach another device: no remote copies, remote signals or barrier semaphores. Data moves between devices by JAX's collectives and lax.ppermute only.
A program may use at most 64 MiB of HBM per device.

```python
import jax
import jax.numpy as jnp

C = 16384
WCOL = 32
TOKENS = 9600
N_CHAN = 4


def set_ends(drawn, stream_key, smallest, largest):
    longest = drawn.shape.index(max(drawn.shape))
    spots = []
    for shift in (0, 1):
        where = [jax.random.randint(jax.random.fold_in(stream_key, axis), (), 0, length) for axis, length in enumerate(drawn.shape)]
        where[longest] = (where[longest] + shift) % drawn.shape[longest]
        spots.append(tuple(where))
    return drawn.at[spots[0]].set(smallest).at[spots[1]].set(largest)


def shard_levels(stream_key, shape, cuts, least, top_value):
    loudness, own = 1.0, jax.random.fold_in(stream_key, 6)
    for dim, blocks in cuts:
        steps = jnp.exp(jax.random.uniform(jax.random.fold_in(own, dim), (blocks,), jnp.float32, least / len(cuts), top_value / len(cuts)))
        loudness = loudness * jnp.repeat(steps, shape[dim] // blocks).reshape([-1 if axis == dim else 1 for axis in range(len(shape))])
    return loudness


def bell_draw(own_key, dims, deviation, limit, shards=(), kind=jnp.bfloat16):
    factor_of = shard_levels(own_key, dims, shards, -0.22, 0.18) if shards else 1.0
    values = jax.random.normal(own_key, dims, jnp.float32) * deviation * factor_of
    return jnp.minimum(jnp.maximum(values, -limit), limit).astype(kind)


def setup_inputs(seed: int = 0) -> dict:
    keys = jax.random.split(jax.random.key(seed), 4)
    return {
        "codes": bell_draw(keys[0], (TOKENS, C), 1.0, 6.0, ((0, 8), (1, 4))),
        "scale_exp": set_ends(jax.random.randint(keys[1], (C,), -2, 3), jax.random.fold_in(keys[1], 1), -2, 2).astype(jnp.int32),
        "delta": bell_draw(keys[2], (TOKENS, C), 0.5, 4.0, ((0, 8), (1, 4))),
    }


def reference(codes, scale_exp, delta):
    scale = jnp.exp2(scale_exp.astype(jnp.float32)).astype(jnp.bfloat16)
    xq = codes * scale[None, :]
    rows = xq.shape[0]
    win = xq.reshape(rows, N_CHAN, C // N_CHAN)[:, :, :WCOL].reshape(rows, WCOL * N_CHAN)
    gram = jnp.dot(xq.T, win, preferred_element_type=jnp.float32) / jnp.float32(TOKENS)
    mismatch = jnp.dot(delta.T, win, preferred_element_type=jnp.float32) / jnp.sqrt(jnp.float32(TOKENS))
    return (gram, mismatch)
```

```python
import functools

import jax
import jax.numpy as jnp
from jax import lax
from jax.experimental import pallas as pl
from jax.experimental.pallas import tpu as pltpu
from jax.sharding import PartitionSpec as P

WCOL = 32
LANES = 128
STEPS = 256.0
TOP = 32760.0
TINY = 1e-36
PIECES = ((0, 0, 2), (0, 2, 2), (1, 0, 2), (1, 2, 2))


def cross(left, right):
    return lax.dot_general(
        left, right, (((0,), (0,)), ((), ())), preferred_element_type=jnp.float32
    )


def plain(codes, scale_exp, delta):
    scale = jnp.exp2(scale_exp.astype(jnp.float32)).astype(jnp.bfloat16)
    xq = codes * scale[None, :]
    total = codes.shape[0] * lax.axis_size("tok")
    piece = lax.all_gather(xq[:, :WCOL], "chan", axis=1, tiled=True)
    both = jnp.stack([cross(xq, piece), cross(delta, piece)])
    summed = lax.psum_scatter(both, "tok", scatter_dimension=1, tiled=True)
    total = jnp.float32(total)
    return (summed[0] * (1.0 / total), summed[1] * (1.0 / jnp.sqrt(total)))


def whole(shape):
    return pl.BlockSpec(shape, lambda *_: (0,) * len(shape))


def steps_of(v):
    top = jnp.maximum(jnp.max(jnp.abs(v), axis=0, keepdims=True), TINY)
    return jnp.ceil(jnp.log2(top) * STEPS) + 1.0


def encode(v, steps):
    scaled = v * (jnp.exp2(steps * (-1.0 / STEPS)) * TOP)
    return jnp.round(scaled).astype(jnp.int32).astype(jnp.int16)


def decode(code, steps):
    unit = jnp.exp2(steps * (1.0 / STEPS)) * (1.0 / TOP)
    return code.astype(jnp.int32).astype(jnp.float32) * unit


def pad16(n):
    return -(-n // 16) * 16


def win_kernel(codes_ref, exp_ref, out_ref):
    scale = jnp.exp2(exp_ref[0:1, :].astype(jnp.float32))
    rows = lax.broadcasted_iota(jnp.int32, (WCOL, LANES), 0)
    cols = lax.broadcasted_iota(jnp.int32, (WCOL, LANES), 1)
    pick = jnp.where(rows == cols, scale, 0.0).astype(jnp.bfloat16)
    out = lax.dot_general(
        pick, codes_ref[...], (((1,), (1,)), ((), ())), preferred_element_type=jnp.float32
    )
    out_ref[...] = out.astype(jnp.bfloat16)


def send_kernel(tiles, groups, t_ref, win_ref, x_ref, out_ref, steps_ref):
    m = pl.program_id(0)

    @pl.when(m == 0)
    def _():
        steps_ref[...] = jnp.zeros_like(steps_ref)

    part = jnp.dot(win_ref[...], x_ref[...], preferred_element_type=jnp.float32)
    w = win_ref.shape[0]
    for j in range(tiles):
        v = part[:, j * LANES : (j + 1) * LANES]
        steps = steps_of(v)
        out_ref[pl.ds(pl.multiple_of((m * tiles + j) * w, w), w), :] = encode(v, steps)
        steps_ref[pl.ds(m * tiles + j, 1), :] = steps

    @pl.when(m == groups - 1)
    def _():
        out_ref[groups * tiles * w :, :] = (
            steps_ref[...].astype(jnp.int32).astype(jnp.int16)
        )


def keep_kernel(tiles, t_ref, win_ref, x_ref, out_ref):
    part = jnp.dot(win_ref[...], x_ref[...], preferred_element_type=jnp.float32)
    w = win_ref.shape[0]
    for j in range(tiles):
        out_ref[j * w : (j + 1) * w, :] = part[:, j * LANES : (j + 1) * LANES]


def middle_kernel(tiles, groups, w, got_ref, keep_ref, own_ref, *send_refs):
    all_steps = got_ref[groups * tiles * w :, :].astype(jnp.int32).astype(jnp.float32)
    fill = jnp.zeros((pad16(tiles) - tiles, LANES), jnp.float32)
    for m in range(groups):
        sent = []
        for j in range(tiles):
            i = m * tiles + j
            rows = slice(i * w, (i + 1) * w)
            v = keep_ref[rows, :] + decode(got_ref[rows, :], all_steps[i : i + 1, :])
            mine = slice(j * w, (j + 1) * w)
            if m == 0:
                own_ref[mine, :] = v
            else:
                steps = steps_of(v)
                send_refs[m - 1][mine, :] = encode(v, steps)
                sent.append(steps)
        if m:
            send_refs[m - 1][tiles * w :, :] = (
                jnp.concatenate(sent + [fill], axis=0).astype(jnp.int32).astype(jnp.int16)
            )


def last_kernel(pieces, groups, w, factors, t_ref, exp_ref, *refs):
    ins, outs = refs[:-2], refs[-2:]
    per_owner = outs[0].shape[0] // LANES
    for p, (stat, first, tiles) in enumerate(pieces):
        own, *got = ins[p * groups : (p + 1) * groups]
        all_steps = [g[tiles * w :, :].astype(jnp.int32).astype(jnp.float32) for g in got]
        for j in range(tiles):
            rows = slice(j * w, (j + 1) * w)
            v = own[rows, :]
            for g, s in zip(got, all_steps):
                v = v + decode(g[rows, :], s[j : j + 1, :])
            factor = jnp.full((1, LANES), factors[stat], jnp.float32)
            if stat == 0:
                e = exp_ref[pl.ds(t_ref[0] * per_owner + first + j, 1), :]
                factor = factor * jnp.exp2(e.astype(jnp.float32))
            at = first + j
            outs[stat][at * LANES : (at + 1) * LANES, :] = (v * factor).T


def shards(codes, scale_exp, delta):
    n = lax.axis_size("tok")
    tokens, chans = codes.shape
    w = WCOL * lax.axis_size("chan")
    groups, owned = n // 2, chans // n
    exps = scale_exp.reshape(chans // LANES, LANES)
    t = lax.axis_index("tok").reshape(1)
    factors = (1.0 / (tokens * n), 1.0 / float(tokens * n) ** 0.5)

    mine = pl.pallas_call(
        win_kernel,
        grid=(1,),
        in_specs=[whole((tokens, LANES)), whole(exps.shape)],
        out_specs=whole((WCOL, tokens)),
        out_shape=jax.ShapeDtypeStruct((WCOL, tokens), jnp.bfloat16),
        name="window",
    )(codes, exps)
    win = lax.all_gather(mine, "chan", axis=0, tiled=True)

    def part(kernel, piece, side, out_rows, out_type, block_rows, scratch, name):
        stat, first, tiles = piece
        per_owner = owned // (LANES * tiles)

        def x_at(m, t_ref):
            return 0, lax.bitwise_xor(t_ref[0], 2 * m + side) * per_owner + first // tiles

        return pl.pallas_call(
            kernel,
            grid_spec=pltpu.PrefetchScalarGridSpec(
                num_scalar_prefetch=1,
                grid=(groups,),
                in_specs=[
                    whole((w, tokens)),
                    pl.BlockSpec((tokens, tiles * LANES), x_at),
                ],
                out_specs=pl.BlockSpec(
                    (block_rows, LANES),
                    lambda m, t_ref: (0 if block_rows == out_rows else m, 0),
                ),
                scratch_shapes=scratch,
            ),
            out_shape=jax.ShapeDtypeStruct((out_rows, LANES), out_type),
            cost_estimate=pl.CostEstimate(
                flops=2 * w * tokens * groups * tiles * LANES,
                bytes_accessed=2 * tokens * groups * tiles * LANES,
                transcendentals=0,
            ),
            name=name,
        )(t, win, (codes, delta)[stat])

    def shift(x, by):
        return lax.ppermute(x, "tok", [(i, i ^ by) for i in range(n)])

    got = []
    for piece in PIECES:
        tiles = piece[2]
        blocks = groups * tiles
        rows = blocks * w + pad16(blocks)
        sent = part(
            functools.partial(send_kernel, tiles, groups), piece, 1, rows, jnp.int16, rows,
            [pltpu.VMEM((pad16(blocks), LANES), jnp.float32)], "send",
        )
        got.append(shift(sent, 1))

    ins = []
    for piece, one in zip(PIECES, got):
        tiles = piece[2]
        blocks = groups * tiles
        kept = part(
            functools.partial(keep_kernel, tiles), piece, 0, blocks * w, jnp.float32,
            tiles * w, [], "keep",
        )
        rows = tiles * w + pad16(tiles)
        own, *sends = pl.pallas_call(
            functools.partial(middle_kernel, tiles, groups, w),
            out_shape=[jax.ShapeDtypeStruct((tiles * w, LANES), jnp.float32)]
            + [jax.ShapeDtypeStruct((rows, LANES), jnp.int16)] * (groups - 1),
            name="middle",
        )(one, kept)
        ins.append(own)
        ins += [shift(s, 2 * m) for m, s in enumerate(sends, 1)]

    out = jax.ShapeDtypeStruct((owned, w), jnp.float32)
    return tuple(
        pl.pallas_call(
            functools.partial(last_kernel, PIECES, groups, w, factors),
            in_specs=[pl.BlockSpec(memory_space=pltpu.SMEM)]
            + [pl.BlockSpec(memory_space=pltpu.VMEM)] * (1 + len(ins)),
            out_shape=[out, out],
            name="last",
        )(t, exps, *ins)
    )


def solution(mesh):
    n, chans = mesh.shape["tok"], mesh.shape["chan"]

    def body(codes, scale_exp, delta):
        local = codes.shape[1]
        fits = (
            n >= 4
            and n & (n - 1) == 0
            and local == n * 4 * LANES
            and WCOL * chans == LANES
        )
        return (shards if fits else plain)(codes, scale_exp, delta)

    in_specs = (P("tok", "chan"), P("chan"), P("tok", "chan"))
    out_specs = (P(("chan", "tok"), None), P(("chan", "tok"), None))
    return jax.shard_map(
        body, mesh=mesh, in_specs=in_specs, out_specs=out_specs, check_vma=False
    )
```

```python
import functools

import jax
import jax.numpy as jnp
from jax import lax
from jax.experimental import pallas as pl
from jax.experimental.pallas import tpu as pltpu
from jax.sharding import PartitionSpec as P

WCOL = 32
LANES = 128
STEPS = 256.0
TOP = 32760.0
TINY = 1e-36
PIECES = ((0, 0, 2), (0, 2, 2), (1, 0, 2), (1, 2, 2))


def cross(left, right):
    return lax.dot_general(
        left, right, (((0,), (0,)), ((), ())), preferred_element_type=jnp.float32
    )


def plain(codes, scale_exp, delta):
    scale = jnp.exp2(scale_exp.astype(jnp.float32)).astype(jnp.bfloat16)
    xq = codes * scale[None, :]
    total = codes.shape[0] * lax.axis_size("tok")
    piece = lax.all_gather(xq[:, :WCOL], "chan", axis=1, tiled=True)
    both = jnp.stack([cross(xq, piece), cross(delta, piece)])
    summed = lax.psum_scatter(both, "tok", scatter_dimension=1, tiled=True)
    total = jnp.float32(total)
    return (summed[0] * (1.0 / total), summed[1] * (1.0 / jnp.sqrt(total)))


def whole(shape):
    return pl.BlockSpec(shape, lambda *_: (0,) * len(shape))


def steps_of(v):
    top = jnp.maximum(jnp.max(jnp.abs(v), axis=0, keepdims=True), TINY)
    return jnp.ceil(jnp.log2(top) * STEPS) + 1.0


def encode(v, steps):
    scaled = v * (jnp.exp2(steps * (-1.0 / STEPS)) * TOP)
    return jnp.round(scaled).astype(jnp.int32).astype(jnp.int16)


def decode(code, steps):
    unit = jnp.exp2(steps * (1.0 / STEPS)) * (1.0 / TOP)
    return code.astype(jnp.int32).astype(jnp.float32) * unit


def pad16(n):
    return -(-n // 16) * 16


def rows16(rows):
    fill = [jnp.zeros((pad16(len(rows)) - len(rows), LANES), jnp.float32)]
    rows = jnp.concatenate(rows + fill if fill[0].shape[0] else rows, axis=0)
    return rows.astype(jnp.int32).astype(jnp.int16)


def call(kernel, out_shape, n_smem, n_vmem, name, flops=0, grant=16):
    return pl.pallas_call(
        kernel,
        out_shape=out_shape,
        in_specs=[pl.BlockSpec(memory_space=pltpu.SMEM)] * n_smem
        + [pl.BlockSpec(memory_space=pltpu.VMEM)] * n_vmem,
        compiler_params=pltpu.CompilerParams(vmem_limit_bytes=grant << 20),
        cost_estimate=pl.CostEstimate(flops=flops, bytes_accessed=0, transcendentals=0),
        name=name,
    )


def win_kernel(codes_ref, exp_ref, out_ref):
    scale = jnp.exp2(exp_ref[0:1, :].astype(jnp.float32))
    rows = lax.broadcasted_iota(jnp.int32, (WCOL, LANES), 0)
    cols = lax.broadcasted_iota(jnp.int32, (WCOL, LANES), 1)
    pick = jnp.where(rows == cols, scale, 0.0).astype(jnp.bfloat16)
    out = lax.dot_general(
        pick, codes_ref[...], (((1,), (1,)), ((), ())), preferred_element_type=jnp.float32
    )
    out_ref[...] = out.astype(jnp.bfloat16)


def send_kernel(piece, owned, groups, t_ref, win_ref, x_ref, out_ref):
    _, first, tiles = piece
    w = win_ref.shape[0]
    every = []
    for m in range(groups):
        owner = lax.bitwise_xor(t_ref[0], 2 * m + 1)
        at = pl.multiple_of(owner * owned + first * LANES, LANES)
        part = jnp.dot(
            win_ref[...], x_ref[:, pl.ds(at, tiles * LANES)], preferred_element_type=jnp.float32
        )
        for j in range(tiles):
            v = part[:, j * LANES : (j + 1) * LANES]
            steps = steps_of(v)
            i = m * tiles + j
            out_ref[i * w : (i + 1) * w, :] = encode(v, steps)
            every.append(steps)
    out_ref[groups * tiles * w :, :] = rows16(every)


def keep_kernel(pieces, owned, groups, t_ref, win_ref, x_ref, *out_refs):
    w = win_ref.shape[0]
    for m in range(groups):
        owner = lax.bitwise_xor(t_ref[0], 2 * m)
        at = pl.multiple_of(owner * owned, LANES)
        part = jnp.dot(
            win_ref[...], x_ref[:, pl.ds(at, owned)], preferred_element_type=jnp.float32
        )
        for (_, first, tiles), out_ref in zip(pieces, out_refs):
            for j in range(tiles):
                i = m * tiles + j
                out_ref[i * w : (i + 1) * w, :] = part[
                    :, (first + j) * LANES : (first + j + 1) * LANES
                ]


def middle_kernel(tiles, groups, w, got_ref, keep_ref, own_ref, *send_refs):
    all_steps = got_ref[groups * tiles * w :, :].astype(jnp.int32).astype(jnp.float32)
    for m in range(groups):
        sent = []
        for j in range(tiles):
            i = m * tiles + j
            rows = slice(i * w, (i + 1) * w)
            v = keep_ref[rows, :] + decode(got_ref[rows, :], all_steps[i : i + 1, :])
            mine = slice(j * w, (j + 1) * w)
            if m == 0:
                own_ref[mine, :] = v
            else:
                steps = steps_of(v)
                send_refs[m - 1][mine, :] = encode(v, steps)
                sent.append(steps)
        if m:
            send_refs[m - 1][tiles * w :, :] = rows16(sent)


def last_kernel(pieces, groups, w, factors, t_ref, exp_ref, *refs):
    ins, outs = refs[:-2], refs[-2:]
    per_owner = outs[0].shape[0] // LANES
    for p, (stat, first, tiles) in enumerate(pieces):
        own, *got = ins[p * groups : (p + 1) * groups]
        all_steps = [g[tiles * w :, :].astype(jnp.int32).astype(jnp.float32) for g in got]
        for j in range(tiles):
            rows = slice(j * w, (j + 1) * w)
            v = own[rows, :]
            for g, s in zip(got, all_steps):
                v = v + decode(g[rows, :], s[j : j + 1, :])
            factor = jnp.full((1, LANES), factors[stat], jnp.float32)
            if stat == 0:
                e = exp_ref[pl.ds(t_ref[0] * per_owner + first + j, 1), :]
                factor = factor * jnp.exp2(e.astype(jnp.float32))
            at = first + j
            outs[stat][at * LANES : (at + 1) * LANES, :] = (v * factor).T


def shards(codes, scale_exp, delta):
    n = lax.axis_size("tok")
    tokens, chans = codes.shape
    w = WCOL * lax.axis_size("chan")
    groups, owned = n // 2, chans // n
    exps = scale_exp.reshape(chans // LANES, LANES)
    t = lax.axis_index("tok").reshape(1)
    factors = (1.0 / (tokens * n), 1.0 / float(tokens * n) ** 0.5)

    mine = pl.pallas_call(
        win_kernel,
        grid=(1,),
        in_specs=[whole((tokens, LANES)), whole(exps.shape)],
        out_specs=whole((WCOL, tokens)),
        out_shape=jax.ShapeDtypeStruct((WCOL, tokens), jnp.bfloat16),
        name="window",
    )(codes, exps)
    win = lax.all_gather(mine, "chan", axis=0, tiled=True)

    def shift(x, by):
        return lax.ppermute(x, "tok", [(i, i ^ by) for i in range(n)])

    inputs = (codes, delta)
    got = []
    for piece in PIECES:
        stat, _, tiles = piece
        blocks = groups * tiles
        sent = call(
            functools.partial(send_kernel, piece, owned, groups),
            jax.ShapeDtypeStruct((blocks * w + pad16(blocks), LANES), jnp.int16),
            1, 2, "send", 2 * w * tokens * blocks * LANES,
        )(t, win, inputs[stat])
        got.append(shift(sent, 1))
    late, _ = lax.optimization_barrier((win, sent))
    kept = {}
    for stat, x in enumerate(inputs):
        mine = [p for p in PIECES if p[0] == stat]
        outs = call(
            functools.partial(keep_kernel, mine, owned, groups),
            [jax.ShapeDtypeStruct((groups * p[2] * w, LANES), jnp.float32) for p in mine],
            1, 2, "keep", 2 * w * tokens * groups * owned,
        )(t, late, x)
        kept.update(zip(mine, outs))

    ins = []
    for piece, one in zip(PIECES, got):
        tiles = piece[2]
        rows = tiles * w + pad16(tiles)
        own, *sends = call(
            functools.partial(middle_kernel, tiles, groups, w),
            [jax.ShapeDtypeStruct((tiles * w, LANES), jnp.float32)]
            + [jax.ShapeDtypeStruct((rows, LANES), jnp.int16)] * (groups - 1),
            0, 2, "middle",
        )(one, kept[piece])
        ins.append(own)
        ins += [shift(s, 2 * m) for m, s in enumerate(sends, 1)]

    out = jax.ShapeDtypeStruct((owned, w), jnp.float32)
    return tuple(
        call(
            functools.partial(last_kernel, PIECES, groups, w, factors),
            [out, out], 1, 1 + len(ins), "last",
        )(t, exps, *ins)
    )


def solution(mesh):
    n, chans = mesh.shape["tok"], mesh.shape["chan"]

    def body(codes, scale_exp, delta):
        local = codes.shape[1]
        fits = (
            n >= 4
            and n & (n - 1) == 0
            and local == n * 4 * LANES
            and WCOL * chans == LANES
        )
        return (shards if fits else plain)(codes, scale_exp, delta)

    in_specs = (P("tok", "chan"), P("chan"), P("tok", "chan"))
    out_specs = (P(("chan", "tok"), None), P(("chan", "tok"), None))
    return jax.shard_map(
        body, mesh=mesh, in_specs=in_specs, out_specs=out_specs, check_vma=False
    )
```
